32 devices in a mesh: ctx: 16 (over z, x, core), head: 2 (over y).
Axes of the slice: x: 2, y: 2, z: 4, core: 2. Of those that a mesh axis runs over, the one named last changes fastest.
Arguments:
- tokens: bfloat16 [4096, 4096], P('ctx', 'head'), may hold values from -19.8 to 19.8
- query_weight: bfloat16 [4096, 4096], P('ctx', 'head'), may hold values from -0.09375 to 0.09375
- key_weight: bfloat16 [4096, 4096], P('ctx', 'head'), may hold values from -0.09375 to 0.09375
- value_weight: bfloat16 [4096, 4096], P('ctx', 'head'), may hold values from -0.09375 to 0.09375
- output_weight: bfloat16 [4096, 4096], P('ctx', 'head'), may hold values from -0.29882812 to 0.29882812
- adapter_down: bfloat16 [3, 8, 4096], replicated, may hold values from -0.09375 to 0.09375
- adapter_up: bfloat16 [3, 8, 4096], P(None, None, 'head'), may hold values from -0.8984375 to 0.8984375
Outputs:
- attended: bfloat16 [4096, 4096], P('ctx', 'head')
The draws below stay inside these ranges and needn't reach their ends.
All inputs are finite; a program needn't handle non-finite values.
Results may differ from the reference program's by a relative error of at most 0.012.
Values may be sent and summed in bfloat16 or wider, within the bound.
No kernel may reach another device: no remote copies, remote signals or barrier semaphores. Data moves between devices by JAX's collectives and lax.ppermute only.
A program may use at most 128 MiB of HBM per device.

```python
import jax
import jax.numpy as jnp
from jax import lax

D = 4096
HEADS = 32
RANK = 8
GROUP_DEV = 16
TOK_DEV = 256
TOKENS = 4096


def common_weight(key):
    normal_part = jax.random.normal(jax.random.fold_in(key, 11), (D, D), jnp.float32)
    return jnp.clip(normal_part, -6.0, 6.0) * D ** (-0.5)


def draw_query_weight(key, part):
    return common_weight(key).astype(jnp.bfloat16)


def draw_key_weight(key, part):
    own_part = jnp.clip(jax.random.normal(jax.random.fold_in(key, 23), (D, D), jnp.float32), -6.0, 6.0) * D ** (-0.5)
    return own_part.astype(jnp.bfloat16)


def draw_tokens(key, part):
    drawn = jnp.clip(jax.random.normal(jax.random.fold_in(key, 31), (TOKENS, D), jnp.float32), -6.0, 6.0)
    return drawn.astype(jnp.bfloat16)


def steps_of(key, dims, split, smallest, high):
    level, own = 1.0, jax.random.fold_in(key, 6)
    for axis_at, blocks in split:
        heights = jnp.exp(jax.random.uniform(jax.random.fold_in(own, axis_at), (blocks,), jnp.float32, smallest / len(split), high / len(split)))
        level = level * jnp.repeat(heights, dims[axis_at] // blocks).reshape([-1 if axis == axis_at else 1 for axis in range(len(dims))])
    return level


def bell_draw(rng, shape, deviation, reach, cuts=(), kind=jnp.bfloat16):
    values = jax.random.normal(rng, shape, jnp.float32) * deviation
    if len(cuts) > 0:
        values = steps_of(rng, shape, cuts, -0.22, 0.18) * values
    return jnp.clip(values, min=-reach, max=reach).astype(kind)


def setup_inputs(seed: int = 0) -> dict:
    key_of = jax.random.split(jax.random.key(seed), 8)
    tokens = draw_tokens(jax.random.fold_in(key_of[7], 71), 0)
    query_weight = draw_query_weight(jax.random.fold_in(key_of[7], 71), 0)
    key_weight = draw_key_weight(jax.random.fold_in(key_of[7], 71), 0)
    value_weight = bell_draw(key_of[3], (D, D), D ** -0.5, 0.09375, ((0, 16), (1, 2)))
    output_weight = bell_draw(key_of[4], (D, D), 0.05, 0.29882812, ((0, 16), (1, 2)))
    adapter_down = bell_draw(key_of[5], (3, RANK, D), D ** -0.5, 0.09375)
    adapter_up = bell_draw(key_of[6], (3, RANK, D), 0.15, 0.8984375, ((2, 2),))
    return {"tokens": tokens, "query_weight": query_weight, "key_weight": key_weight, "value_weight": value_weight, "output_weight": output_weight, "adapter_down": adapter_down, "adapter_up": adapter_up}


def rotary(projection, positions):
    half_dim = projection.shape[-1] // 2
    inverse_freq = 10000.0 ** (-(jnp.arange(half_dim, dtype=jnp.float32) * 2.0) / projection.shape[-1])
    angles = positions.astype(jnp.float32)[:, None] * inverse_freq[None, :]
    cosine = jnp.cos(angles)[:, None, :]
    sine_part = jnp.sin(angles)[:, None, :]
    first_half = projection[..., :half_dim]
    second = projection[..., half_dim:]
    return jnp.concatenate([first_half * cosine - second * sine_part, second * cosine + first_half * sine_part], -1)


def reference(tokens, query_weight, key_weight, value_weight, output_weight, adapter_down, adapter_up):
    head_dim = D // HEADS
    positions = jnp.arange(TOKENS, dtype=jnp.int32)
    projected = []
    for which, weight in enumerate((query_weight, key_weight, value_weight)):
        base_proj = jnp.dot(tokens, weight, preferred_element_type=jnp.float32)
        low_rank = jnp.dot(tokens, adapter_down[which].T, preferred_element_type=jnp.float32).astype(jnp.bfloat16)
        full_proj = base_proj + 2.0 * jnp.dot(low_rank, adapter_up[which], preferred_element_type=jnp.float32)
        projected.append(full_proj.reshape(TOKENS, HEADS, head_dim))
    query = rotary(projected[0], positions).astype(jnp.bfloat16)
    key_rot = rotary(projected[1], positions).astype(jnp.bfloat16)
    value = projected[2].astype(jnp.bfloat16)
    group_size = GROUP_DEV * TOK_DEV
    shift_span = group_size // 2
    shifted = (jnp.arange(HEADS) >= HEADS // 2)[None, :, None]

    def rolled(array, amount):
        return jnp.where(shifted, jnp.roll(array, amount, axis=0), array)

    groups = TOKENS // group_size

    def arrange(array):
        array = rolled(array, -shift_span)
        return array.reshape(groups, group_size, HEADS, head_dim).transpose(0, 2, 1, 3).reshape(groups * HEADS, group_size, head_dim)

    causal = jnp.arange(group_size)[:, None] >= jnp.arange(group_size)[None, :]
    scale = head_dim ** -0.5

    def attend(triple):
        query_blk, key_blk, value_blk = triple
        scores = jnp.dot(query_blk, key_blk.T, preferred_element_type=jnp.float32) * scale
        scores = jnp.where(causal, scores, -1e30)
        row_max = jnp.max(scores, axis=-1, keepdims=True)
        weights = jnp.where(causal, jnp.exp(scores - row_max), 0.0)
        denominator = jnp.sum(weights, axis=-1, keepdims=True)
        result = jnp.dot(weights.astype(jnp.bfloat16), value_blk, preferred_element_type=jnp.float32) / denominator
        return result.astype(jnp.bfloat16)

    outputs = lax.map(attend, (arrange(query), arrange(key_rot), arrange(value)))
    outputs = outputs.reshape(groups, HEADS, group_size, head_dim).transpose(0, 2, 1, 3).reshape(TOKENS, HEADS, head_dim)
    merged = rolled(outputs, shift_span).reshape(TOKENS, D)
    return jnp.dot(merged, output_weight, preferred_element_type=jnp.float32).astype(jnp.bfloat16)
```

```python
import functools

import jax
import jax.numpy as jnp
from jax import lax
from jax.experimental import pallas as pl
from jax.experimental.pallas import tpu as pltpu
from jax.sharding import PartitionSpec as P

D = 4096
HEADS = 32
GROUP_DEV = 16


def shifted(x, axis, by):
    peers = lax.axis_size(axis)
    return lax.ppermute(x, axis, [(i, (i + by) % peers) for i in range(peers)])


def rotary(projection, positions):
    half_dim = projection.shape[-1] // 2
    inverse_freq = 10000.0 ** (
        -(jnp.arange(half_dim, dtype=jnp.float32) * 2.0) / projection.shape[-1]
    )
    angles = positions.astype(jnp.float32)[:, None] * inverse_freq[None, :]
    cosine = jnp.cos(angles)[:, None, :]
    sine_part = jnp.sin(angles)[:, None, :]
    first_half = projection[..., :half_dim]
    second = projection[..., half_dim:]
    return jnp.concatenate(
        [first_half * cosine - second * sine_part, second * cosine + first_half * sine_part], -1
    )


def fold_rows(left_side, weight_piece):
    return jnp.dot(left_side, weight_piece, preferred_element_type=jnp.float32)


def update_block(carry, query, key_blk, value_blk, key_place, query_pos, group_size):
    row_max, denominator, running = carry
    scale = query.shape[-1] ** (-0.5)
    scores = jnp.einsum("qhd,khd->hqk", query, key_blk, preferred_element_type=jnp.float32) * scale
    allowed = ((query_pos // group_size)[:, None] == (key_place // group_size)[None, :]) & (
        key_place[None, :] <= query_pos[:, None]
    )
    scores = jnp.where(allowed[None], scores, -1e30)
    new_max = jnp.maximum(row_max, jnp.max(scores, axis=-1))
    weights = jnp.where(allowed[None], jnp.exp(scores - new_max[..., None]), 0.0)
    factor = jnp.exp(row_max - new_max)
    denominator = denominator * factor + jnp.sum(weights, axis=-1)
    running = running * factor[..., None] + jnp.einsum(
        "hqk,khd->hqd", weights.astype(jnp.bfloat16), value_blk, preferred_element_type=jnp.float32
    )
    return (new_max, denominator, running)


def per_device(
    tokens, query_weight, key_weight, value_weight, output_weight, adapter_down, adapter_up
):
    tok_rows = tokens.shape[0]
    ctx_count = lax.axis_size("ctx")
    ctx_index = lax.axis_index("ctx")
    head_count = lax.axis_size("head")
    heads_dev = HEADS // head_count
    head_dim = D // HEADS
    slab_len = tok_rows * ctx_count
    group_size = GROUP_DEV * tok_rows
    shift_span = group_size // 2
    shifted_dev = lax.axis_index("head") >= head_count // 2
    features = lax.all_gather(tokens, "head", axis=1, tiled=True)

    def fold_one(weight_piece):
        return fold_rows(features, weight_piece)

    projected = (
        fold_one(lax.all_gather(query_weight, "ctx", axis=0, tiled=True)),
        fold_one(lax.all_gather(key_weight, "ctx", axis=0, tiled=True)),
        fold_one(lax.all_gather(value_weight, "ctx", axis=0, tiled=True)),
    )
    low_ranks = jnp.einsum(
        "td,jrd->jtr", features, adapter_down, preferred_element_type=jnp.float32
    ).astype(jnp.bfloat16)
    local_rows = jnp.arange(tok_rows, dtype=jnp.int32)
    positions = ctx_index * tok_rows + local_rows
    full_projs = []
    for which in range(3):
        full_proj = projected[which] + 2.0 * jnp.dot(
            low_ranks[which], adapter_up[which], preferred_element_type=jnp.float32
        )
        full_projs.append(full_proj.reshape(tok_rows, heads_dev, head_dim))
    query = rotary(full_projs[0], positions).astype(jnp.bfloat16)
    key_rot = rotary(full_projs[1], positions).astype(jnp.bfloat16)
    value = full_projs[2].astype(jnp.bfloat16)
    key_value = jnp.stack([key_rot, value])
    offset = jnp.where(shifted_dev, shift_span, 0).astype(jnp.int32)
    query_pos = (positions - offset) % slab_len
    start_carry = (
        jnp.full((heads_dev, tok_rows), -1e30, jnp.float32),
        jnp.zeros((heads_dev, tok_rows), jnp.float32),
        jnp.zeros((heads_dev, tok_rows, head_dim), jnp.float32),
    )
    carry = update_block(start_carry, query, key_rot, value, query_pos, query_pos, group_size)

    def one_turn(turn, state):
        current, running_carry = state
        current = shifted(current, "ctx", 1)
        source = (ctx_index - turn - 1) % ctx_count
        key_place = (source * tok_rows + local_rows - offset) % slab_len
        running_carry = update_block(
            running_carry, query, current[0], current[1], key_place, query_pos, group_size
        )
        return (current, running_carry)

    unused, carry = lax.fori_loop(0, GROUP_DEV - 1, one_turn, (key_value, carry))
    row_max, denominator, running = carry
    result = (running / denominator[..., None]).astype(jnp.bfloat16)
    result = result.transpose(1, 0, 2).reshape(tok_rows, heads_dev * head_dim)
    merged = lax.all_gather(result, "head", axis=1, tiled=True)
    attended = fold_rows(merged, lax.all_gather(output_weight, "ctx", axis=0, tiled=True))
    return attended.astype(jnp.bfloat16)


def exchanged(x, axis, bit):
    peers = lax.axis_size(axis)
    return lax.ppermute(x, axis, [(i, i ^ bit) for i in range(peers)])


def sent(x, pairs):
    return lax.ppermute(x, "ctx", pairs)


def line_gather(own, plane):
    z_index = lax.axis_index("ctx") // plane

    def hops(steps):
        return [(a * plane + i, b * plane + i) for a, b in steps for i in range(plane)]

    inner = (z_index == 1) | (z_index == 2)
    middle = hops([(1, 2), (2, 1)])
    outward = hops([(1, 0), (2, 3)])
    near = sent(own, hops([(0, 1), (1, 0), (2, 3), (3, 2)]))
    first = sent(own, middle)
    first_out = sent(first, outward)
    far = sent(near, middle)
    far_out = sent(far, outward)
    return [own, near, jnp.where(inner, first, first_out), jnp.where(inner, far, far_out)]


def line_sources(z_index):
    low = z_index < 2
    return [z_index, z_index ^ 1, jnp.where(low, 2, 1), jnp.where(low, 3, 0)]


def flash_kernel(table, *refs, head_dim, block, piece):
    own, peer, out = refs[:4], refs[4:8], refs[8]
    query, key, value = refs[9:]
    slab_len = query.shape[0]
    entry = 0
    for slot in range(4):
        for part in range(own[slot].shape[0] // piece):
            rows = slice(part * piece, (part + 1) * piece)
            for source in (own[slot], peer[slot]):
                place = pl.ds(pl.multiple_of(table[entry] * piece, piece), piece)
                query[place, :] = source[rows, :head_dim]
                key[place, :] = source[rows, head_dim : 2 * head_dim]
                value[place, :] = source[rows, 2 * head_dim :]
                entry += 1
    offset = table[entry]
    scale = head_dim ** (-0.5) * 1.4426950408889634
    diagonal = lax.broadcasted_iota(jnp.int32, (block, block), 1) <= lax.broadcasted_iota(
        jnp.int32, (block, block), 0
    )
    contract = (((1,), (1,)), ((), ()))
    for step in range(slab_len // block):
        rows = slice(step * block, (step + 1) * block)
        q_blk = query[rows, :]
        corner = lax.dot_general(q_blk, key[rows, :], contract, preferred_element_type=jnp.float32)
        corner = jnp.where(diagonal, corner, -1e30)
        top = jnp.max(corner, axis=-1, keepdims=True)
        if step:
            before = lax.dot_general(
                q_blk, key[: step * block, :], contract, preferred_element_type=jnp.float32
            )
            top = jnp.maximum(top, jnp.max(before, axis=-1, keepdims=True))
        weights = jnp.exp2((corner - top) * scale)
        total = jnp.sum(weights, axis=-1, keepdims=True)
        mixed = jnp.dot(
            weights.astype(jnp.bfloat16), value[rows, :], preferred_element_type=jnp.float32
        )
        if step:
            weights = jnp.exp2((before - top) * scale)
            total += jnp.sum(weights, axis=-1, keepdims=True)
            mixed += jnp.dot(
                weights.astype(jnp.bfloat16),
                value[: step * block, :],
                preferred_element_type=jnp.float32,
            )
        start = lax.rem(offset + step * block, slab_len)
        out[pl.ds(pl.multiple_of(start, block), block), :] = (mixed / total).astype(jnp.bfloat16)


def flash(table, own, peer, slab_len, head_dim, piece, block=256):
    body = functools.partial(flash_kernel, head_dim=head_dim, block=block, piece=piece)
    vmem = pl.BlockSpec(memory_space=pltpu.VMEM)
    scratch = [pltpu.VMEM((slab_len, head_dim), jnp.bfloat16)] * 3
    return pl.pallas_call(
        body,
        out_shape=jax.ShapeDtypeStruct((slab_len, head_dim), jnp.bfloat16),
        in_specs=[pl.BlockSpec(memory_space=pltpu.SMEM)] + [vmem] * 8,
        out_specs=vmem,
        scratch_shapes=scratch,
        compiler_params=pltpu.CompilerParams(vmem_limit_bytes=48 * 2**20),
        name="flash",
    )(table, *own, *peer)


def one_head_per_device(
    tokens, query_weight, key_weight, value_weight, output_weight, adapter_down, adapter_up
):
    tok_rows = tokens.shape[0]
    ctx_count = lax.axis_size("ctx")
    ctx_index = lax.axis_index("ctx")
    y_index = lax.axis_index("head")
    head_dim = D // HEADS
    slab_len = tok_rows * ctx_count
    plane = ctx_count // 4
    half = tok_rows // 2
    z_index, in_plane = ctx_index // plane, ctx_index % plane
    rank = adapter_down.shape[1]

    kept = lax.dynamic_slice_in_dim(tokens, y_index * half, half, 0)
    other = lax.dynamic_slice_in_dim(tokens, (1 - y_index) * half, half, 0)
    came = exchanged(other, "head", 1)
    shard = jnp.where(
        y_index == 0, jnp.concatenate([kept, came], 1), jnp.concatenate([came, kept], 1)
    )
    line = line_gather(shard, plane)
    slots = []
    for piece in line:
        across = exchanged(piece, "ctx", 2)
        slots.append([piece, exchanged(piece, "ctx", 1), across, exchanged(across, "ctx", 1)])

    pair_weights = []
    for weight in (query_weight, key_weight, value_weight):
        mine = lax.all_to_all(weight, "ctx", split_axis=1, concat_axis=0, tiled=True)
        pair_weights.append(jnp.concatenate([mine, exchanged(mine, "head", 1)], 1))

    down = adapter_down.reshape(3 * rank, D)
    up_mine = lax.dynamic_slice_in_dim(adapter_up, ctx_index * head_dim, head_dim, 2)
    up_pair = jnp.concatenate([up_mine, exchanged(up_mine, "head", 1)], 2)

    variant = jnp.array([0, 1, 2, 3], dtype=jnp.int32)
    local = jnp.arange(half, dtype=jnp.int32)
    own_parts, peer_parts, places = [], [], []
    for slot, source_z in zip(slots, line_sources(z_index)):
        rows = jnp.concatenate(slot, 0)
        sources = source_z * plane + (in_plane ^ variant)
        places.append(sources)
        positions = (sources[:, None] * tok_rows + y_index * half + local[None, :]).reshape(-1)
        low = lax.dot_general(
            rows, down, (((1,), (1,)), ((), ())), preferred_element_type=jnp.float32
        ).astype(jnp.bfloat16)
        outs = []
        for which in range(3):
            proj = fold_rows(rows, pair_weights[which]) + 2.0 * fold_rows(
                low[:, which * rank : (which + 1) * rank], up_pair[which]
            )
            proj = proj.reshape(rows.shape[0], 2, head_dim)
            if which < 2:
                proj = rotary(proj, positions)
            outs.append(proj.astype(jnp.bfloat16))
        own_parts.append(jnp.concatenate([out[:, 0] for out in outs], 1))
        peer_parts.append(exchanged(jnp.concatenate([out[:, 1] for out in outs], 1), "head", 1))

    shift = jnp.where(y_index * ctx_count + ctx_index >= HEADS // 2, slab_len // 2, 0)
    sides = jnp.stack([y_index, 1 - y_index]).astype(jnp.int32)
    table = (jnp.concatenate(places)[:, None] * 2 + sides[None, :]).reshape(-1)
    table = (table - shift // half) % (slab_len // half)
    table = jnp.concatenate([table, shift[None]]).astype(jnp.int32)
    result = flash(table, own_parts, peer_parts, slab_len, head_dim, half)
    mixed = lax.all_to_all(result, "ctx", split_axis=0, concat_axis=1, tiled=True)
    mixed_other = exchanged(mixed, "head", 1)

    tied, unused = lax.optimization_barrier((output_weight, slots[3][2]))
    full = jnp.zeros((D, output_weight.shape[1]), jnp.bfloat16)
    for piece, source_z in zip(line_gather(tied, plane), line_sources(z_index)):
        across = exchanged(piece, "ctx", 2)
        group = [piece, exchanged(piece, "ctx", 1), across, exchanged(across, "ctx", 1)]
        for bits, block in enumerate(group):
            start = (source_z * plane + (in_plane ^ bits)) * tok_rows
            full = lax.dynamic_update_slice_in_dim(full, block, start, 0)
    width = mixed.shape[1]
    attended = fold_rows(mixed, lax.dynamic_slice_in_dim(full, y_index * width, width, 0))
    attended += fold_rows(
        mixed_other, lax.dynamic_slice_in_dim(full, (1 - y_index) * width, width, 0)
    )
    return attended.astype(jnp.bfloat16)


def one_head_fits(mesh):
    ctx_count, head_count = mesh.shape["ctx"], mesh.shape["head"]
    return ctx_count == GROUP_DEV and ctx_count // 4 == 4 and HEADS == ctx_count * head_count and head_count == 2


def solution(mesh):
    body = one_head_per_device if one_head_fits(mesh) else per_device
    in_specs = (
        P("ctx", "head"),
        P("ctx", "head"),
        P("ctx", "head"),
        P("ctx", "head"),
        P("ctx", "head"),
        P(),
        P(None, None, "head"),
    )
    out_specs = P("ctx", "head")
    return jax.shard_map(
        body, mesh=mesh, in_specs=in_specs, out_specs=out_specs, check_vma=False
    )
```

```python
import functools

import jax
import jax.numpy as jnp
from jax import lax
from jax.experimental import pallas as pl
from jax.experimental.pallas import tpu as pltpu
from jax.sharding import PartitionSpec as P

D = 4096
HEADS = 32
GROUP_DEV = 16


def shifted(x, axis, by):
    peers = lax.axis_size(axis)
    return lax.ppermute(x, axis, [(i, (i + by) % peers) for i in range(peers)])


def rotary(projection, positions):
    half_dim = projection.shape[-1] // 2
    inverse_freq = 10000.0 ** (
        -(jnp.arange(half_dim, dtype=jnp.float32) * 2.0) / projection.shape[-1]
    )
    angles = positions.astype(jnp.float32)[:, None] * inverse_freq[None, :]
    cosine = jnp.cos(angles)[:, None, :]
    sine_part = jnp.sin(angles)[:, None, :]
    first_half = projection[..., :half_dim]
    second = projection[..., half_dim:]
    return jnp.concatenate(
        [first_half * cosine - second * sine_part, second * cosine + first_half * sine_part], -1
    )


def fold_rows(left_side, weight_piece):
    return jnp.dot(left_side, weight_piece, preferred_element_type=jnp.float32)


def update_block(carry, query, key_blk, value_blk, key_place, query_pos, group_size):
    row_max, denominator, running = carry
    scale = query.shape[-1] ** (-0.5)
    scores = jnp.einsum("qhd,khd->hqk", query, key_blk, preferred_element_type=jnp.float32) * scale
    allowed = ((query_pos // group_size)[:, None] == (key_place // group_size)[None, :]) & (
        key_place[None, :] <= query_pos[:, None]
    )
    scores = jnp.where(allowed[None], scores, -1e30)
    new_max = jnp.maximum(row_max, jnp.max(scores, axis=-1))
    weights = jnp.where(allowed[None], jnp.exp(scores - new_max[..., None]), 0.0)
    factor = jnp.exp(row_max - new_max)
    denominator = denominator * factor + jnp.sum(weights, axis=-1)
    running = running * factor[..., None] + jnp.einsum(
        "hqk,khd->hqd", weights.astype(jnp.bfloat16), value_blk, preferred_element_type=jnp.float32
    )
    return (new_max, denominator, running)


def per_device(
    tokens, query_weight, key_weight, value_weight, output_weight, adapter_down, adapter_up
):
    tok_rows = tokens.shape[0]
    ctx_count = lax.axis_size("ctx")
    ctx_index = lax.axis_index("ctx")
    head_count = lax.axis_size("head")
    heads_dev = HEADS // head_count
    head_dim = D // HEADS
    slab_len = tok_rows * ctx_count
    group_size = GROUP_DEV * tok_rows
    shift_span = group_size // 2
    shifted_dev = lax.axis_index("head") >= head_count // 2
    features = lax.all_gather(tokens, "head", axis=1, tiled=True)

    def fold_one(weight_piece):
        return fold_rows(features, weight_piece)

    projected = (
        fold_one(lax.all_gather(query_weight, "ctx", axis=0, tiled=True)),
        fold_one(lax.all_gather(key_weight, "ctx", axis=0, tiled=True)),
        fold_one(lax.all_gather(value_weight, "ctx", axis=0, tiled=True)),
    )
    low_ranks = jnp.einsum(
        "td,jrd->jtr", features, adapter_down, preferred_element_type=jnp.float32
    ).astype(jnp.bfloat16)
    local_rows = jnp.arange(tok_rows, dtype=jnp.int32)
    positions = ctx_index * tok_rows + local_rows
    full_projs = []
    for which in range(3):
        full_proj = projected[which] + 2.0 * jnp.dot(
            low_ranks[which], adapter_up[which], preferred_element_type=jnp.float32
        )
        full_projs.append(full_proj.reshape(tok_rows, heads_dev, head_dim))
    query = rotary(full_projs[0], positions).astype(jnp.bfloat16)
    key_rot = rotary(full_projs[1], positions).astype(jnp.bfloat16)
    value = full_projs[2].astype(jnp.bfloat16)
    key_value = jnp.stack([key_rot, value])
    offset = jnp.where(shifted_dev, shift_span, 0).astype(jnp.int32)
    query_pos = (positions - offset) % slab_len
    start_carry = (
        jnp.full((heads_dev, tok_rows), -1e30, jnp.float32),
        jnp.zeros((heads_dev, tok_rows), jnp.float32),
        jnp.zeros((heads_dev, tok_rows, head_dim), jnp.float32),
    )
    carry = update_block(start_carry, query, key_rot, value, query_pos, query_pos, group_size)

    def one_turn(turn, state):
        current, running_carry = state
        current = shifted(current, "ctx", 1)
        source = (ctx_index - turn - 1) % ctx_count
        key_place = (source * tok_rows + local_rows - offset) % slab_len
        running_carry = update_block(
            running_carry, query, current[0], current[1], key_place, query_pos, group_size
        )
        return (current, running_carry)

    _, carry = lax.fori_loop(0, GROUP_DEV - 1, one_turn, (key_value, carry))
    _, denominator, running = carry
    result = (running / denominator[..., None]).astype(jnp.bfloat16)
    result = result.transpose(1, 0, 2).reshape(tok_rows, heads_dev * head_dim)
    merged = lax.all_gather(result, "head", axis=1, tiled=True)
    attended = fold_rows(merged, lax.all_gather(output_weight, "ctx", axis=0, tiled=True))
    return attended.astype(jnp.bfloat16)


def exchanged(x, axis, bit):
    peers = lax.axis_size(axis)
    return lax.ppermute(x, axis, [(i, i ^ bit) for i in range(peers)])


def sent(x, pairs):
    return lax.ppermute(x, "ctx", pairs)


def line_gather(own, plane):
    z_index = lax.axis_index("ctx") // plane

    def hops(steps):
        return [(a * plane + i, b * plane + i) for a, b in steps for i in range(plane)]

    inner = (z_index == 1) | (z_index == 2)
    middle = hops([(1, 2), (2, 1)])
    outward = hops([(1, 0), (2, 3)])
    near = sent(own, hops([(0, 1), (1, 0), (2, 3), (3, 2)]))
    first = sent(own, middle)
    first_out = sent(first, outward)
    far = sent(near, middle)
    far_out = sent(far, outward)
    return [own, near, jnp.where(inner, first, first_out), jnp.where(inner, far, far_out)]


def line_sources(z_index):
    low = z_index < 2
    return [z_index, z_index ^ 1, jnp.where(low, 2, 1), jnp.where(low, 3, 0)]


def flash_kernel(table, *refs, head_dim, block, piece):
    *parts, out, query, key, value = refs
    own, peer = parts[: len(parts) // 2], parts[len(parts) // 2 :]
    slab_len = query.shape[0]
    entry = 0
    for pair in zip(own, peer):
        for part in range(pair[0].shape[0] // piece):
            rows = slice(part * piece, (part + 1) * piece)
            for source in pair:
                place = pl.ds(pl.multiple_of(table[entry] * piece, piece), piece)
                query[place, :] = source[rows, :head_dim]
                key[place, :] = source[rows, head_dim : 2 * head_dim]
                value[place, :] = source[rows, 2 * head_dim :]
                entry += 1
    offset = table[entry]
    scale = head_dim ** (-0.5) * 1.4426950408889634
    diagonal = lax.broadcasted_iota(jnp.int32, (block, block), 1) <= lax.broadcasted_iota(
        jnp.int32, (block, block), 0
    )
    contract = (((1,), (1,)), ((), ()))
    for step in range(slab_len // block):
        rows = slice(step * block, (step + 1) * block)
        q_blk = query[rows, :]
        corner = lax.dot_general(q_blk, key[rows, :], contract, preferred_element_type=jnp.float32)
        corner = jnp.where(diagonal, corner, -1e30)
        top = jnp.max(corner, axis=-1, keepdims=True)
        if step:
            before = lax.dot_general(
                q_blk, key[: step * block, :], contract, preferred_element_type=jnp.float32
            )
            top = jnp.maximum(top, jnp.max(before, axis=-1, keepdims=True))
        weights = jnp.exp2((corner - top) * scale)
        total = jnp.sum(weights, axis=-1, keepdims=True)
        mixed = jnp.dot(
            weights.astype(jnp.bfloat16), value[rows, :], preferred_element_type=jnp.float32
        )
        if step:
            weights = jnp.exp2((before - top) * scale)
            total += jnp.sum(weights, axis=-1, keepdims=True)
            mixed += jnp.dot(
                weights.astype(jnp.bfloat16),
                value[: step * block, :],
                preferred_element_type=jnp.float32,
            )
        start = lax.rem(offset + step * block, slab_len)
        out[pl.ds(pl.multiple_of(start, block), block), :] = (mixed / total).astype(jnp.bfloat16)


def flash(table, own, peer, slab_len, head_dim, piece, block=256):
    body = functools.partial(flash_kernel, head_dim=head_dim, block=block, piece=piece)
    vmem = pl.BlockSpec(memory_space=pltpu.VMEM)
    scratch = [pltpu.VMEM((slab_len, head_dim), jnp.bfloat16)] * 3
    return pl.pallas_call(
        body,
        out_shape=jax.ShapeDtypeStruct((slab_len, head_dim), jnp.bfloat16),
        in_specs=[pl.BlockSpec(memory_space=pltpu.SMEM)] + [vmem] * (2 * len(own)),
        out_specs=vmem,
        scratch_shapes=scratch,
        compiler_params=pltpu.CompilerParams(vmem_limit_bytes=48 * 2**20),
        name="flash",
    )(table, *own, *peer)


def project_kernel(*refs, head_dim):
    *inputs, down, up, cosine, sine, mine, other, total = refs
    pieces, weights = inputs[:-6], inputs[-6:]
    step = pl.program_id(0)
    rows = jnp.concatenate([piece[...] for piece in pieces], 0)

    @pl.when(step == 0)
    def _():
        total[...] = jnp.zeros_like(total)

    wide = 2 * head_dim
    for which in range(3):
        pair = jnp.concatenate([weights[which][...], weights[which + 3][...]], 1)
        total[:, which * wide : (which + 1) * wide] += fold_rows(rows, pair)
    total[:, 3 * wide :] += fold_rows(rows, down[...])

    @pl.when(step == pl.num_programs(0) - 1)
    def _():
        low = total[:, 3 * wide :].astype(jnp.bfloat16)
        for which in range(3):
            for side, out in enumerate((mine, other)):
                start = which * wide + side * head_dim
                proj = total[:, start : start + head_dim] + 2.0 * fold_rows(
                    low, up[:, start : start + head_dim]
                )
                if which < 2:
                    turned = pltpu.roll(proj, head_dim // 2, 1)
                    proj = proj * cosine[...] + turned * sine[...]
                out[:, which * head_dim : (which + 1) * head_dim] = proj.astype(jnp.bfloat16)


def project(pieces, weights, down, up, cosine, sine, head_dim, depth=1024):
    rows = sum(piece.shape[0] for piece in pieces)
    width = weights[0].shape[0]
    whole = lambda shape: pl.BlockSpec(shape, lambda k: (0, 0))
    out = jax.ShapeDtypeStruct((rows, 3 * head_dim), jnp.bfloat16)
    return pl.pallas_call(
        functools.partial(project_kernel, head_dim=head_dim),
        grid=(width // depth,),
        out_shape=(out, out),
        in_specs=[pl.BlockSpec((piece.shape[0], depth), lambda k: (0, k)) for piece in pieces]
        + [pl.BlockSpec((depth, head_dim), lambda k: (k, 0))] * 6
        + [pl.BlockSpec((depth, down.shape[1]), lambda k: (k, 0))]
        + [whole(up.shape), whole(cosine.shape), whole(sine.shape)],
        out_specs=[whole(out.shape)] * 2,
        scratch_shapes=[pltpu.VMEM((rows, 6 * head_dim + down.shape[1]), jnp.float32)],
        compiler_params=pltpu.CompilerParams(vmem_limit_bytes=40 * 2**20),
        name="project",
    )(*pieces, *weights, down, up, cosine, sine)


def output_kernel(table, *refs):
    *pieces, mine, other, out, heads, left = refs
    count, _, head_dim = mine.shape

    @pl.when(pl.program_id(0) == 0)
    def _():
        first = table[len(pieces)]
        heads[pl.ds(first, count)] = mine[...]
        heads[pl.ds(count - first, count)] = other[...]
        for at in range(2 * count):
            piece, inner = divmod(at * head_dim, pieces[0].shape[0])
            head = table[piece] * (pieces[0].shape[0] // head_dim) + inner // head_dim
            left[:, at * head_dim : (at + 1) * head_dim] = heads[head]

    weight = jnp.concatenate([piece[...] for piece in pieces], 0)
    out[...] = fold_rows(left[...], weight).astype(jnp.bfloat16)


def output_project(table, pieces, mine, other, wide=256):
    count, rows, head_dim = mine.shape
    cols = pieces[0].shape[1]
    part = pl.BlockSpec((pieces[0].shape[0], wide), lambda n: (0, n))
    whole = pl.BlockSpec(mine.shape, lambda n: (0, 0, 0))
    return pl.pallas_call(
        output_kernel,
        grid=(cols // wide,),
        out_shape=jax.ShapeDtypeStruct((rows, cols), jnp.bfloat16),
        in_specs=[pl.BlockSpec(memory_space=pltpu.SMEM)] + [part] * len(pieces) + [whole] * 2,
        out_specs=pl.BlockSpec((rows, wide), lambda n: (0, n)),
        scratch_shapes=[
            pltpu.VMEM((2 * count, rows, head_dim), jnp.bfloat16),
            pltpu.VMEM((rows, 2 * count * head_dim), jnp.bfloat16),
        ],
        compiler_params=pltpu.CompilerParams(vmem_limit_bytes=40 * 2**20),
        name="output",
    )(table, *pieces, mine, other)


def one_head_per_device(*args):
    return attention_layer(*args)


def attention_layer(
    tokens, query_weight, key_weight, value_weight, output_weight, adapter_down, adapter_up
):
    tok_rows = tokens.shape[0]
    ctx_count = lax.axis_size("ctx")
    ctx_index = lax.axis_index("ctx")
    y_index = lax.axis_index("head")
    head_dim = D // HEADS
    slab_len = tok_rows * ctx_count
    plane = ctx_count // 4
    half = tok_rows // 2
    z_index, in_plane = ctx_index // plane, ctx_index % plane
    rank = adapter_down.shape[1]

    kept = lax.dynamic_slice_in_dim(tokens, y_index * half, half, 0)
    other = lax.dynamic_slice_in_dim(tokens, (1 - y_index) * half, half, 0)
    came = exchanged(other, "head", 1)
    shard = jnp.where(
        y_index == 0, jnp.concatenate([kept, came], 1), jnp.concatenate([came, kept], 1)
    )

    def spread(own):
        line = line_gather(own, plane)
        groups = []
        for piece in line:
            across = exchanged(piece, "ctx", 2)
            beside = exchanged(piece, "ctx", 1)
            groups.append([piece, beside, across, exchanged(across, "ctx", 1)])
        return groups

    slots = spread(shard)

    def swap(weight):
        return lax.all_to_all(weight, "ctx", split_axis=1, concat_axis=0, tiled=True)

    mine = [swap(weight) for weight in (query_weight, key_weight, value_weight)]
    pair_weights = mine + [exchanged(weight, "head", 1) for weight in mine]

    down = jnp.pad(adapter_down.reshape(3 * rank, D).T, ((0, 0), (0, head_dim - 3 * rank)))
    up_mine = lax.dynamic_slice_in_dim(adapter_up, ctx_index * head_dim, head_dim, 2)
    up_pair = jnp.concatenate([up_mine, exchanged(up_mine, "head", 1)], 2)
    up = jnp.zeros((head_dim, 6 * head_dim), jnp.bfloat16)
    for which in range(3):
        up = lax.dynamic_update_slice(up, up_pair[which], (which * rank, which * 2 * head_dim))

    variant = jnp.array([0, 1, 2, 3], dtype=jnp.int32)
    local = jnp.arange(half, dtype=jnp.int32)
    inverse_freq = 10000.0 ** (-(jnp.arange(head_dim // 2, dtype=jnp.float32) * 2.0) / head_dim)
    places = [z * plane + (in_plane ^ variant) for z in line_sources(z_index)]
    own_parts, peer_parts = [], []
    for first, last in GROUPS:
        rows_from = jnp.concatenate(places[first:last])[:, None] * tok_rows
        positions = (rows_from + y_index * half + local[None, :]).reshape(-1)
        angles = positions.astype(jnp.float32)[:, None] * inverse_freq[None, :]
        cosine, sine = jnp.cos(angles), jnp.sin(angles)
        cosine = jnp.concatenate([cosine, cosine], 1)
        sine = jnp.concatenate([-sine, sine], 1)
        pieces = [piece for slot in slots[first:last] for piece in slot]
        own_part, peer_part = project(pieces, pair_weights, down, up, cosine, sine, head_dim)
        own_parts.append(own_part)
        peer_parts.append(exchanged(peer_part, "head", 1))

    sources = jnp.concatenate(places)
    shift = jnp.where(y_index * ctx_count + ctx_index >= HEADS // 2, slab_len // 2, 0)
    sides = jnp.stack([y_index, 1 - y_index]).astype(jnp.int32)
    table = (sources[:, None] * 2 + sides[None, :]).reshape(-1)
    table = (table - shift // half) % (slab_len // half)
    table = jnp.concatenate([table, shift[None]]).astype(jnp.int32)
    result = flash(table, own_parts, peer_parts, slab_len, head_dim, half)
    blocks = result.reshape(ctx_count, tok_rows, head_dim)
    mixed = lax.all_to_all(blocks, "ctx", split_axis=0, concat_axis=0, tiled=True)
    mixed_other = exchanged(mixed, "head", 1)

    pieces = [piece for group in spread(output_weight) for piece in group]
    heads_first = y_index * ctx_count
    out_table = jnp.concatenate([sources, heads_first[None]]).astype(jnp.int32)
    return output_project(out_table, pieces, mixed, mixed_other)


GROUPS = ((0, 3), (3, 4))


def one_head_fits(mesh):
    ctx_count, head_count = mesh.shape["ctx"], mesh.shape["head"]
    return ctx_count == GROUP_DEV and ctx_count // 4 == 4 and HEADS == ctx_count * head_count and head_count == 2


def solution(mesh):
    fits = one_head_fits(mesh)
    body = one_head_per_device if fits else per_device
    in_specs = (
        P("ctx", "head"),
        P("ctx", "head"),
        P("ctx", "head"),
        P("ctx", "head"),
        P("ctx", "head"),
        P(),
        P(None, None, "head"),
    )
    out_specs = P("ctx", "head")
    return jax.shard_map(
        body, mesh=mesh, in_specs=in_specs, out_specs=out_specs, check_vma=False
    )
```

```python
import functools

import jax
import jax.numpy as jnp
from jax import lax
from jax.experimental import pallas as pl
from jax.experimental.pallas import tpu as pltpu
from jax.sharding import PartitionSpec as P

D = 4096
HEADS = 32
GROUP_DEV = 16


def shifted(x, axis, by):
    peers = lax.axis_size(axis)
    return lax.ppermute(x, axis, [(i, (i + by) % peers) for i in range(peers)])


def rotary(projection, positions):
    half_dim = projection.shape[-1] // 2
    inverse_freq = 10000.0 ** (
        -(jnp.arange(half_dim, dtype=jnp.float32) * 2.0) / projection.shape[-1]
    )
    angles = positions.astype(jnp.float32)[:, None] * inverse_freq[None, :]
    cosine = jnp.cos(angles)[:, None, :]
    sine_part = jnp.sin(angles)[:, None, :]
    first_half = projection[..., :half_dim]
    second = projection[..., half_dim:]
    return jnp.concatenate(
        [first_half * cosine - second * sine_part, second * cosine + first_half * sine_part], -1
    )


def fold_rows(left_side, weight_piece):
    return jnp.dot(left_side, weight_piece, preferred_element_type=jnp.float32)


def update_block(carry, query, key_blk, value_blk, key_place, query_pos, group_size):
    row_max, denominator, running = carry
    scale = query.shape[-1] ** (-0.5)
    scores = jnp.einsum("qhd,khd->hqk", query, key_blk, preferred_element_type=jnp.float32) * scale
    allowed = ((query_pos // group_size)[:, None] == (key_place // group_size)[None, :]) & (
        key_place[None, :] <= query_pos[:, None]
    )
    scores = jnp.where(allowed[None], scores, -1e30)
    new_max = jnp.maximum(row_max, jnp.max(scores, axis=-1))
    weights = jnp.where(allowed[None], jnp.exp(scores - new_max[..., None]), 0.0)
    factor = jnp.exp(row_max - new_max)
    denominator = denominator * factor + jnp.sum(weights, axis=-1)
    running = running * factor[..., None] + jnp.einsum(
        "hqk,khd->hqd", weights.astype(jnp.bfloat16), value_blk, preferred_element_type=jnp.float32
    )
    return (new_max, denominator, running)


def per_device(
    tokens, query_weight, key_weight, value_weight, output_weight, adapter_down, adapter_up
):
    tok_rows = tokens.shape[0]
    ctx_count = lax.axis_size("ctx")
    ctx_index = lax.axis_index("ctx")
    head_count = lax.axis_size("head")
    heads_dev = HEADS // head_count
    head_dim = D // HEADS
    slab_len = tok_rows * ctx_count
    group_size = GROUP_DEV * tok_rows
    shift_span = group_size // 2
    shifted_dev = lax.axis_index("head") >= head_count // 2
    features = lax.all_gather(tokens, "head", axis=1, tiled=True)

    def fold_one(weight_piece):
        return fold_rows(features, weight_piece)

    projected = (
        fold_one(lax.all_gather(query_weight, "ctx", axis=0, tiled=True)),
        fold_one(lax.all_gather(key_weight, "ctx", axis=0, tiled=True)),
        fold_one(lax.all_gather(value_weight, "ctx", axis=0, tiled=True)),
    )
    low_ranks = jnp.einsum(
        "td,jrd->jtr", features, adapter_down, preferred_element_type=jnp.float32
    ).astype(jnp.bfloat16)
    local_rows = jnp.arange(tok_rows, dtype=jnp.int32)
    positions = ctx_index * tok_rows + local_rows
    full_projs = []
    for which in range(3):
        full_proj = projected[which] + 2.0 * jnp.dot(
            low_ranks[which], adapter_up[which], preferred_element_type=jnp.float32
        )
        full_projs.append(full_proj.reshape(tok_rows, heads_dev, head_dim))
    query = rotary(full_projs[0], positions).astype(jnp.bfloat16)
    key_rot = rotary(full_projs[1], positions).astype(jnp.bfloat16)
    value = full_projs[2].astype(jnp.bfloat16)
    key_value = jnp.stack([key_rot, value])
    offset = jnp.where(shifted_dev, shift_span, 0).astype(jnp.int32)
    query_pos = (positions - offset) % slab_len
    start_carry = (
        jnp.full((heads_dev, tok_rows), -1e30, jnp.float32),
        jnp.zeros((heads_dev, tok_rows), jnp.float32),
        jnp.zeros((heads_dev, tok_rows, head_dim), jnp.float32),
    )
    carry = update_block(start_carry, query, key_rot, value, query_pos, query_pos, group_size)

    def one_turn(turn, state):
        current, running_carry = state
        current = shifted(current, "ctx", 1)
        source = (ctx_index - turn - 1) % ctx_count
        key_place = (source * tok_rows + local_rows - offset) % slab_len
        running_carry = update_block(
            running_carry, query, current[0], current[1], key_place, query_pos, group_size
        )
        return (current, running_carry)

    _, carry = lax.fori_loop(0, GROUP_DEV - 1, one_turn, (key_value, carry))
    _, denominator, running = carry
    result = (running / denominator[..., None]).astype(jnp.bfloat16)
    result = result.transpose(1, 0, 2).reshape(tok_rows, heads_dev * head_dim)
    merged = lax.all_gather(result, "head", axis=1, tiled=True)
    attended = fold_rows(merged, lax.all_gather(output_weight, "ctx", axis=0, tiled=True))
    return attended.astype(jnp.bfloat16)


def exchanged(x, axis, bit):
    peers = lax.axis_size(axis)
    return lax.ppermute(x, axis, [(i, i ^ bit) for i in range(peers)])


def sent(x, pairs):
    return lax.ppermute(x, "ctx", pairs)


def line_gather(own, plane):
    z_index = lax.axis_index("ctx") // plane

    def hops(steps):
        return [(a * plane + i, b * plane + i) for a, b in steps for i in range(plane)]

    inner = (z_index == 1) | (z_index == 2)
    middle = hops([(1, 2), (2, 1)])
    outward = hops([(1, 0), (2, 3)])
    near = sent(own, hops([(0, 1), (1, 0), (2, 3), (3, 2)]))
    first = sent(own, middle)
    first_out = sent(first, outward)
    far = sent(near, middle)
    far_out = sent(far, outward)
    return [own, near, jnp.where(inner, first, first_out), jnp.where(inner, far, far_out)]


def line_sources(z_index):
    low = z_index < 2
    return [z_index, z_index ^ 1, jnp.where(low, 2, 1), jnp.where(low, 3, 0)]


def flash_kernel(table, *refs, plan, head_dim, block, piece):
    *parts, out, query, key, value = refs
    targets = (query, key, value)
    slab_len = query.shape[0]
    for at, (first, kinds) in enumerate(plan):
        for part in range(parts[2 * at].shape[0] // piece):
            rows = slice(part * piece, (part + 1) * piece)
            for side in range(2):
                number = table[(first * 4 + part) * 2 + side]
                place = pl.ds(pl.multiple_of(number * piece, piece), piece)
                for inner, kind in enumerate(kinds):
                    columns = slice(inner * head_dim, (inner + 1) * head_dim)
                    targets[kind][place, :] = parts[2 * at + side][rows, columns]
    offset = table[2 * (slab_len // (2 * piece))]
    scale = head_dim ** (-0.5) * 1.4426950408889634
    diagonal = lax.broadcasted_iota(jnp.int32, (block, block), 1) <= lax.broadcasted_iota(
        jnp.int32, (block, block), 0
    )
    contract = (((1,), (1,)), ((), ()))
    for step in range(slab_len // block):
        rows = slice(step * block, (step + 1) * block)
        q_blk = query[rows, :]
        corner = lax.dot_general(q_blk, key[rows, :], contract, preferred_element_type=jnp.float32)
        corner = jnp.where(diagonal, corner, -1e30)
        top = jnp.max(corner, axis=-1, keepdims=True)
        if step:
            before = lax.dot_general(
                q_blk, key[: step * block, :], contract, preferred_element_type=jnp.float32
            )
            top = jnp.maximum(top, jnp.max(before, axis=-1, keepdims=True))
        weights = jnp.exp2((corner - top) * scale)
        total = jnp.sum(weights, axis=-1, keepdims=True)
        mixed = jnp.dot(
            weights.astype(jnp.bfloat16), value[rows, :], preferred_element_type=jnp.float32
        )
        if step:
            weights = jnp.exp2((before - top) * scale)
            total += jnp.sum(weights, axis=-1, keepdims=True)
            mixed += jnp.dot(
                weights.astype(jnp.bfloat16),
                value[: step * block, :],
                preferred_element_type=jnp.float32,
            )
        start = lax.rem(offset + step * block, slab_len)
        out[pl.ds(pl.multiple_of(start, block), block), :] = (mixed / total).astype(jnp.bfloat16)


def flash(table, parts, plan, slab_len, head_dim, piece, block=256):
    body = functools.partial(flash_kernel, plan=plan, head_dim=head_dim, block=block, piece=piece)
    vmem = pl.BlockSpec(memory_space=pltpu.VMEM)
    scratch = [pltpu.VMEM((slab_len, head_dim), jnp.bfloat16)] * 3
    return pl.pallas_call(
        body,
        out_shape=jax.ShapeDtypeStruct((slab_len, head_dim), jnp.bfloat16),
        in_specs=[pl.BlockSpec(memory_space=pltpu.SMEM)] + [vmem] * len(parts),
        out_specs=vmem,
        scratch_shapes=scratch,
        compiler_params=pltpu.CompilerParams(vmem_limit_bytes=48 * 2**20),
        name="flash",
    )(table, *parts)


def project_kernel(*refs, kinds, head_dim):
    *inputs, down, up, cosine, sine, mine, other, total = refs
    count = len(kinds)
    pieces, weights = inputs[: -2 * count], inputs[-2 * count :]
    step = pl.program_id(0)
    rows = jnp.concatenate([piece[...] for piece in pieces], 0)

    @pl.when(step == 0)
    def _():
        total[...] = jnp.zeros_like(total)

    wide = 2 * head_dim
    for which in range(count):
        pair = jnp.concatenate([weights[which][...], weights[which + count][...]], 1)
        total[:, which * wide : (which + 1) * wide] += fold_rows(rows, pair)
    total[:, count * wide :] += fold_rows(rows, down[...])

    @pl.when(step == pl.num_programs(0) - 1)
    def _():
        low = total[:, count * wide :].astype(jnp.bfloat16)
        for which, kind in enumerate(kinds):
            for side, out in enumerate((mine, other)):
                start = which * wide + side * head_dim
                proj = total[:, start : start + head_dim] + 2.0 * fold_rows(
                    low, up[:, kind * wide + side * head_dim : kind * wide + (side + 1) * head_dim]
                )
                if kind < 2:
                    turned = pltpu.roll(proj, head_dim // 2, 1)
                    proj = proj * cosine[...] + turned * sine[...]
                out[:, which * head_dim : (which + 1) * head_dim] = proj.astype(jnp.bfloat16)


def project(pieces, weights, kinds, down, up, cosine, sine, head_dim, depth=512):
    rows = sum(piece.shape[0] for piece in pieces)
    width = weights[0].shape[0]
    whole = lambda shape: pl.BlockSpec(shape, lambda k: (0, 0))
    out = jax.ShapeDtypeStruct((rows, len(kinds) * head_dim), jnp.bfloat16)
    return pl.pallas_call(
        functools.partial(project_kernel, kinds=kinds, head_dim=head_dim),
        grid=(width // depth,),
        out_shape=(out, out),
        in_specs=[pl.BlockSpec((piece.shape[0], depth), lambda k: (0, k)) for piece in pieces]
        + [pl.BlockSpec((depth, head_dim), lambda k: (k, 0))] * len(weights)
        + [pl.BlockSpec((depth, down.shape[1]), lambda k: (k, 0))]
        + [whole(up.shape), whole(cosine.shape), whole(sine.shape)],
        out_specs=[whole(out.shape)] * 2,
        scratch_shapes=[pltpu.VMEM((rows, 2 * len(kinds) * head_dim + down.shape[1]), jnp.float32)],
        compiler_params=pltpu.CompilerParams(vmem_limit_bytes=40 * 2**20),
        name="project",
    )(*pieces, *weights, down, up, cosine, sine)


def output_kernel(table, *refs):
    *pieces, mine, other, out, heads, left = refs
    count, _, head_dim = mine.shape

    @pl.when(pl.program_id(0) == 0)
    def _():
        first = table[len(pieces)]
        heads[pl.ds(first, count)] = mine[...]
        heads[pl.ds(count - first, count)] = other[...]
        for at in range(2 * count):
            piece, inner = divmod(at * head_dim, pieces[0].shape[0])
            head = table[piece] * (pieces[0].shape[0] // head_dim) + inner // head_dim
            left[:, at * head_dim : (at + 1) * head_dim] = heads[head]

    weight = jnp.concatenate([piece[...] for piece in pieces], 0)
    out[...] = fold_rows(left[...], weight).astype(jnp.bfloat16)


def output_project(table, pieces, mine, other, wide=256):
    count, rows, head_dim = mine.shape
    cols = pieces[0].shape[1]
    part = pl.BlockSpec((pieces[0].shape[0], wide), lambda n: (0, n))
    whole = pl.BlockSpec(mine.shape, lambda n: (0, 0, 0))
    return pl.pallas_call(
        output_kernel,
        grid=(cols // wide,),
        out_shape=jax.ShapeDtypeStruct((rows, cols), jnp.bfloat16),
        in_specs=[pl.BlockSpec(memory_space=pltpu.SMEM)] + [part] * len(pieces) + [whole] * 2,
        out_specs=pl.BlockSpec((rows, wide), lambda n: (0, n)),
        scratch_shapes=[
            pltpu.VMEM((2 * count, rows, head_dim), jnp.bfloat16),
            pltpu.VMEM((rows, 2 * count * head_dim), jnp.bfloat16),
        ],
        compiler_params=pltpu.CompilerParams(vmem_limit_bytes=40 * 2**20),
        name="output",
    )(table, *pieces, mine, other)


def one_head_per_device(*args):
    return attention_layer(*args)


def attention_layer(
    tokens, query_weight, key_weight, value_weight, output_weight, adapter_down, adapter_up
):
    tok_rows = tokens.shape[0]
    ctx_count = lax.axis_size("ctx")
    ctx_index = lax.axis_index("ctx")
    y_index = lax.axis_index("head")
    head_dim = D // HEADS
    slab_len = tok_rows * ctx_count
    plane = ctx_count // 4
    half = tok_rows // 2
    z_index, in_plane = ctx_index // plane, ctx_index % plane
    rank = adapter_down.shape[1]

    kept = lax.dynamic_slice_in_dim(tokens, y_index * half, half, 0)
    other = lax.dynamic_slice_in_dim(tokens, (1 - y_index) * half, half, 0)
    came = exchanged(other, "head", 1)
    shard = jnp.where(
        y_index == 0, jnp.concatenate([kept, came], 1), jnp.concatenate([came, kept], 1)
    )

    def spread(own):
        line = line_gather(own, plane)
        groups = []
        for piece in line:
            across = exchanged(piece, "ctx", 2)
            beside = exchanged(piece, "ctx", 1)
            groups.append([piece, beside, across, exchanged(across, "ctx", 1)])
        return groups

    slots = spread(shard)

    def swap(weight):
        return lax.all_to_all(weight, "ctx", split_axis=1, concat_axis=0, tiled=True)

    mine = [swap(weight) for weight in (query_weight, key_weight, value_weight)]
    others = [exchanged(weight, "head", 1) for weight in mine]

    down = jnp.pad(adapter_down.reshape(3 * rank, D).T, ((0, 0), (0, head_dim - 3 * rank)))
    up_mine = lax.dynamic_slice_in_dim(adapter_up, ctx_index * head_dim, head_dim, 2)
    up_pair = jnp.concatenate([up_mine, exchanged(up_mine, "head", 1)], 2)
    up = jnp.zeros((head_dim, 6 * head_dim), jnp.bfloat16)
    for which in range(3):
        up = lax.dynamic_update_slice(up, up_pair[which], (which * rank, which * 2 * head_dim))

    variant = jnp.array([0, 1, 2, 3], dtype=jnp.int32)
    local = jnp.arange(half, dtype=jnp.int32)
    inverse_freq = 10000.0 ** (-(jnp.arange(head_dim // 2, dtype=jnp.float32) * 2.0) / head_dim)
    places = [z * plane + (in_plane ^ variant) for z in line_sources(z_index)]
    parts, plan = [], []
    for first, last, split in GROUPS:
        rows_from = jnp.concatenate(places[first:last])[:, None] * tok_rows
        positions = (rows_from + y_index * half + local[None, :]).reshape(-1)
        angles = positions.astype(jnp.float32)[:, None] * inverse_freq[None, :]
        cosine, sine = jnp.cos(angles), jnp.sin(angles)
        cosine = jnp.concatenate([cosine, cosine], 1)
        sine = jnp.concatenate([-sine, sine], 1)
        pieces = [piece for slot in slots[first:last] for piece in slot]
        for kinds in split:
            weights = [mine[kind] for kind in kinds] + [others[kind] for kind in kinds]
            own_part, peer_part = project(
                pieces, weights, kinds, down, up, cosine, sine, head_dim
            )
            parts += [own_part, exchanged(peer_part, "head", 1)]
            plan.append((first, kinds))

    sources = jnp.concatenate(places)
    shift = jnp.where(y_index * ctx_count + ctx_index >= HEADS // 2, slab_len // 2, 0)
    sides = jnp.stack([y_index, 1 - y_index]).astype(jnp.int32)
    table = (sources[:, None] * 2 + sides[None, :]).reshape(-1)
    table = (table - shift // half) % (slab_len // half)
    table = jnp.concatenate([table, shift[None]]).astype(jnp.int32)
    result = flash(table, parts, plan, slab_len, head_dim, half)
    blocks = result.reshape(ctx_count, tok_rows, head_dim)
    mixed = lax.all_to_all(blocks, "ctx", split_axis=0, concat_axis=0, tiled=True)
    mixed_other = exchanged(mixed, "head", 1)

    pieces = [piece for group in spread(output_weight) for piece in group]
    heads_first = y_index * ctx_count
    out_table = jnp.concatenate([sources, heads_first[None]]).astype(jnp.int32)
    return output_project(out_table, pieces, mixed, mixed_other)


GROUPS = ((0, 3, ((0, 1), (2,))), (3, 4, ((0, 1, 2),)))


def one_head_fits(mesh):
    ctx_count, head_count = mesh.shape["ctx"], mesh.shape["head"]
    return ctx_count == GROUP_DEV and ctx_count // 4 == 4 and HEADS == ctx_count * head_count and head_count == 2


def solution(mesh):
    fits = one_head_fits(mesh)
    body = one_head_per_device if fits else per_device
    in_specs = (
        P("ctx", "head"),
        P("ctx", "head"),
        P("ctx", "head"),
        P("ctx", "head"),
        P("ctx", "head"),
        P(),
        P(None, None, "head"),
    )
    out_specs = P("ctx", "head")
    return jax.shard_map(
        body, mesh=mesh, in_specs=in_specs, out_specs=out_specs, check_vma=False
    )
```

```python
import functools

import jax
import jax.numpy as jnp
from jax import lax
from jax.experimental import pallas as pl
from jax.experimental.pallas import tpu as pltpu
from jax.sharding import PartitionSpec as P

D = 4096
HEADS = 32
GROUP_DEV = 16


def shifted(x, axis, by):
    peers = lax.axis_size(axis)
    return lax.ppermute(x, axis, [(i, (i + by) % peers) for i in range(peers)])


def rotary(projection, positions):
    half_dim = projection.shape[-1] // 2
    inverse_freq = 10000.0 ** (
        -(jnp.arange(half_dim, dtype=jnp.float32) * 2.0) / projection.shape[-1]
    )
    angles = positions.astype(jnp.float32)[:, None] * inverse_freq[None, :]
    cosine = jnp.cos(angles)[:, None, :]
    sine_part = jnp.sin(angles)[:, None, :]
    first_half = projection[..., :half_dim]
    second = projection[..., half_dim:]
    return jnp.concatenate(
        [first_half * cosine - second * sine_part, second * cosine + first_half * sine_part], -1
    )


def fold_rows(left_side, weight_piece):
    return jnp.dot(left_side, weight_piece, preferred_element_type=jnp.float32)


def update_block(carry, query, key_blk, value_blk, key_place, query_pos, group_size):
    row_max, denominator, running = carry
    scale = query.shape[-1] ** (-0.5)
    scores = jnp.einsum("qhd,khd->hqk", query, key_blk, preferred_element_type=jnp.float32) * scale
    allowed = ((query_pos // group_size)[:, None] == (key_place // group_size)[None, :]) & (
        key_place[None, :] <= query_pos[:, None]
    )
    scores = jnp.where(allowed[None], scores, -1e30)
    new_max = jnp.maximum(row_max, jnp.max(scores, axis=-1))
    weights = jnp.where(allowed[None], jnp.exp(scores - new_max[..., None]), 0.0)
    factor = jnp.exp(row_max - new_max)
    denominator = denominator * factor + jnp.sum(weights, axis=-1)
    running = running * factor[..., None] + jnp.einsum(
        "hqk,khd->hqd", weights.astype(jnp.bfloat16), value_blk, preferred_element_type=jnp.float32
    )
    return (new_max, denominator, running)


def per_device(
    tokens, query_weight, key_weight, value_weight, output_weight, adapter_down, adapter_up
):
    tok_rows = tokens.shape[0]
    ctx_count = lax.axis_size("ctx")
    ctx_index = lax.axis_index("ctx")
    head_count = lax.axis_size("head")
    heads_dev = HEADS // head_count
    head_dim = D // HEADS
    slab_len = tok_rows * ctx_count
    group_size = GROUP_DEV * tok_rows
    shift_span = group_size // 2
    shifted_dev = lax.axis_index("head") >= head_count // 2
    features = lax.all_gather(tokens, "head", axis=1, tiled=True)

    def fold_one(weight_piece):
        return fold_rows(features, weight_piece)

    projected = (
        fold_one(lax.all_gather(query_weight, "ctx", axis=0, tiled=True)),
        fold_one(lax.all_gather(key_weight, "ctx", axis=0, tiled=True)),
        fold_one(lax.all_gather(value_weight, "ctx", axis=0, tiled=True)),
    )
    low_ranks = jnp.einsum(
        "td,jrd->jtr", features, adapter_down, preferred_element_type=jnp.float32
    ).astype(jnp.bfloat16)
    local_rows = jnp.arange(tok_rows, dtype=jnp.int32)
    positions = ctx_index * tok_rows + local_rows
    full_projs = []
    for which in range(3):
        full_proj = projected[which] + 2.0 * jnp.dot(
            low_ranks[which], adapter_up[which], preferred_element_type=jnp.float32
        )
        full_projs.append(full_proj.reshape(tok_rows, heads_dev, head_dim))
    query = rotary(full_projs[0], positions).astype(jnp.bfloat16)
    key_rot = rotary(full_projs[1], positions).astype(jnp.bfloat16)
    value = full_projs[2].astype(jnp.bfloat16)
    key_value = jnp.stack([key_rot, value])
    offset = jnp.where(shifted_dev, shift_span, 0).astype(jnp.int32)
    query_pos = (positions - offset) % slab_len
    start_carry = (
        jnp.full((heads_dev, tok_rows), -1e30, jnp.float32),
        jnp.zeros((heads_dev, tok_rows), jnp.float32),
        jnp.zeros((heads_dev, tok_rows, head_dim), jnp.float32),
    )
    carry = update_block(start_carry, query, key_rot, value, query_pos, query_pos, group_size)

    def one_turn(turn, state):
        current, running_carry = state
        current = shifted(current, "ctx", 1)
        source = (ctx_index - turn - 1) % ctx_count
        key_place = (source * tok_rows + local_rows - offset) % slab_len
        running_carry = update_block(
            running_carry, query, current[0], current[1], key_place, query_pos, group_size
        )
        return (current, running_carry)

    _, carry = lax.fori_loop(0, GROUP_DEV - 1, one_turn, (key_value, carry))
    _, denominator, running = carry
    result = (running / denominator[..., None]).astype(jnp.bfloat16)
    result = result.transpose(1, 0, 2).reshape(tok_rows, heads_dev * head_dim)
    merged = lax.all_gather(result, "head", axis=1, tiled=True)
    attended = fold_rows(merged, lax.all_gather(output_weight, "ctx", axis=0, tiled=True))
    return attended.astype(jnp.bfloat16)


def exchanged(x, axis, bit):
    peers = lax.axis_size(axis)
    return lax.ppermute(x, axis, [(i, i ^ bit) for i in range(peers)])


def sent(x, pairs):
    return lax.ppermute(x, "ctx", pairs)


def line_gather(own, plane):
    z_index = lax.axis_index("ctx") // plane

    def hops(steps):
        return [(a * plane + i, b * plane + i) for a, b in steps for i in range(plane)]

    inner = (z_index == 1) | (z_index == 2)
    middle = hops([(1, 2), (2, 1)])
    outward = hops([(1, 0), (2, 3)])
    near = sent(own, hops([(0, 1), (1, 0), (2, 3), (3, 2)]))
    first = sent(own, middle)
    first_out = sent(first, outward)
    far = sent(near, middle)
    far_out = sent(far, outward)
    return [own, near, jnp.where(inner, first, first_out), jnp.where(inner, far, far_out)]


def line_sources(z_index):
    low = z_index < 2
    return [z_index, z_index ^ 1, jnp.where(low, 2, 1), jnp.where(low, 3, 0)]


def flash_kernel(table, *refs, plan, head_dim, block, piece):
    *parts, out, query, key, value = refs
    targets = (query, key, value)
    slab_len = query.shape[0]
    for at, (first, kinds) in enumerate(plan):
        for part in range(parts[2 * at].shape[0] // piece):
            rows = slice(part * piece, (part + 1) * piece)
            for side in range(2):
                number = table[(first * 4 + part) * 2 + side]
                place = pl.ds(pl.multiple_of(number * piece, piece), piece)
                for inner, kind in enumerate(kinds):
                    columns = slice(inner * head_dim, (inner + 1) * head_dim)
                    targets[kind][place, :] = parts[2 * at + side][rows, columns]
    offset = table[2 * (slab_len // (2 * piece))]
    scale = head_dim ** (-0.5) * 1.4426950408889634
    diagonal = lax.broadcasted_iota(jnp.int32, (block, block), 1) <= lax.broadcasted_iota(
        jnp.int32, (block, block), 0
    )
    contract = (((1,), (1,)), ((), ()))
    for step in range(slab_len // block):
        rows = slice(step * block, (step + 1) * block)
        q_blk = query[rows, :]
        corner = lax.dot_general(q_blk, key[rows, :], contract, preferred_element_type=jnp.float32)
        corner = jnp.where(diagonal, corner, -1e30)
        top = jnp.max(corner, axis=-1, keepdims=True)
        if step:
            before = lax.dot_general(
                q_blk, key[: step * block, :], contract, preferred_element_type=jnp.float32
            )
            top = jnp.maximum(top, jnp.max(before, axis=-1, keepdims=True))
        weights = jnp.exp2((corner - top) * scale)
        total = jnp.sum(weights, axis=-1, keepdims=True)
        mixed = jnp.dot(
            weights.astype(jnp.bfloat16), value[rows, :], preferred_element_type=jnp.float32
        )
        if step:
            weights = jnp.exp2((before - top) * scale)
            total += jnp.sum(weights, axis=-1, keepdims=True)
            mixed += jnp.dot(
                weights.astype(jnp.bfloat16),
                value[: step * block, :],
                preferred_element_type=jnp.float32,
            )
        start = lax.rem(offset + step * block, slab_len)
        out[pl.ds(pl.multiple_of(start, block), block), :] = (mixed / total).astype(jnp.bfloat16)


def flash(table, parts, plan, slab_len, head_dim, piece, block=256):
    body = functools.partial(flash_kernel, plan=plan, head_dim=head_dim, block=block, piece=piece)
    vmem = pl.BlockSpec(memory_space=pltpu.VMEM)
    scratch = [pltpu.VMEM((slab_len, head_dim), jnp.bfloat16)] * 3
    return pl.pallas_call(
        body,
        out_shape=jax.ShapeDtypeStruct((slab_len, head_dim), jnp.bfloat16),
        in_specs=[pl.BlockSpec(memory_space=pltpu.SMEM)] + [vmem] * len(parts),
        out_specs=vmem,
        scratch_shapes=scratch,
        compiler_params=pltpu.CompilerParams(vmem_limit_bytes=48 * 2**20),
        name="flash",
    )(table, *parts)


def lower_kernel(*refs):
    *pieces, down, out, total = refs
    step = pl.program_id(0)

    @pl.when(step == 0)
    def _():
        total[...] = jnp.zeros_like(total)

    rows = jnp.concatenate([piece[...] for piece in pieces], 0)
    total[...] += fold_rows(rows, down[...])

    @pl.when(step == pl.num_programs(0) - 1)
    def _():
        out[...] = total[...].astype(jnp.bfloat16)


def lower(pieces, down, depth=512):
    rows = sum(piece.shape[0] for piece in pieces)
    width, rank = down.shape
    return pl.pallas_call(
        lower_kernel,
        grid=(width // depth,),
        out_shape=jax.ShapeDtypeStruct((rows, rank), jnp.bfloat16),
        in_specs=[pl.BlockSpec((piece.shape[0], depth), lambda k: (0, k)) for piece in pieces]
        + [pl.BlockSpec((depth, rank), lambda k: (k, 0))],
        out_specs=pl.BlockSpec((rows, rank), lambda k: (0, 0)),
        scratch_shapes=[pltpu.VMEM((rows, rank), jnp.float32)],
        compiler_params=pltpu.CompilerParams(vmem_limit_bytes=40 * 2**20),
        name="lower",
    )(*pieces, down)


def project_kernel(*refs, kinds, head_dim):
    *inputs, low, up, cosine, sine, mine, other, total = refs
    count = len(kinds)
    pieces, weights = inputs[: -2 * count], inputs[-2 * count :]
    step = pl.program_id(0)
    wide = 2 * head_dim

    @pl.when(step == 0)
    def _():
        total[...] = jnp.zeros_like(total)

    rows = jnp.concatenate([piece[...] for piece in pieces], 0)
    for which in range(count):
        pair = jnp.concatenate([weights[which][...], weights[which + count][...]], 1)
        total[:, which * wide : (which + 1) * wide] += fold_rows(rows, pair)

    @pl.when(step == pl.num_programs(0) - 1)
    def _():
        for which, kind in enumerate(kinds):
            added = fold_rows(low[...], up[:, kind * wide : (kind + 1) * wide])
            for side, out in enumerate((mine, other)):
                start = which * wide + side * head_dim
                proj = total[:, start : start + head_dim]
                proj = proj + 2.0 * added[:, side * head_dim : (side + 1) * head_dim]
                if kind < 2:
                    turned = pltpu.roll(proj, head_dim // 2, 1)
                    proj = proj * cosine[...] + turned * sine[...]
                out[:, which * head_dim : (which + 1) * head_dim] = proj.astype(jnp.bfloat16)


def project(pieces, weights, kinds, low, up, cosine, sine, head_dim, depth):
    rows = sum(piece.shape[0] for piece in pieces)
    width = weights[0].shape[0]
    whole = lambda shape: pl.BlockSpec(shape, lambda k: (0, 0))
    out = jax.ShapeDtypeStruct((rows, len(kinds) * head_dim), jnp.bfloat16)
    return pl.pallas_call(
        functools.partial(project_kernel, kinds=kinds, head_dim=head_dim),
        grid=(width // depth,),
        out_shape=(out, out),
        in_specs=[pl.BlockSpec((piece.shape[0], depth), lambda k: (0, k)) for piece in pieces]
        + [pl.BlockSpec((depth, head_dim), lambda k: (k, 0))] * len(weights)
        + [whole(low.shape), whole(up.shape), whole(cosine.shape), whole(sine.shape)],
        out_specs=[whole(out.shape)] * 2,
        scratch_shapes=[pltpu.VMEM((rows, 2 * len(kinds) * head_dim), jnp.float32)],
        compiler_params=pltpu.CompilerParams(vmem_limit_bytes=40 * 2**20),
        name="project",
    )(*pieces, *weights, low, up, cosine, sine)


def output_kernel(table, *refs):
    *pieces, mine, other, out, heads, left = refs
    count, _, head_dim = mine.shape

    @pl.when(pl.program_id(0) == 0)
    def _():
        first = table[len(pieces)]
        heads[pl.ds(first, count)] = mine[...]
        heads[pl.ds(count - first, count)] = other[...]
        for at in range(2 * count):
            piece, inner = divmod(at * head_dim, pieces[0].shape[0])
            head = table[piece] * (pieces[0].shape[0] // head_dim) + inner // head_dim
            left[:, at * head_dim : (at + 1) * head_dim] = heads[head]

    weight = jnp.concatenate([piece[...] for piece in pieces], 0)
    out[...] = fold_rows(left[...], weight).astype(jnp.bfloat16)


def output_project(table, pieces, mine, other, wide=256):
    count, rows, head_dim = mine.shape
    cols = pieces[0].shape[1]
    part = pl.BlockSpec((pieces[0].shape[0], wide), lambda n: (0, n))
    whole = pl.BlockSpec(mine.shape, lambda n: (0, 0, 0))
    return pl.pallas_call(
        output_kernel,
        grid=(cols // wide,),
        out_shape=jax.ShapeDtypeStruct((rows, cols), jnp.bfloat16),
        in_specs=[pl.BlockSpec(memory_space=pltpu.SMEM)] + [part] * len(pieces) + [whole] * 2,
        out_specs=pl.BlockSpec((rows, wide), lambda n: (0, n)),
        scratch_shapes=[
            pltpu.VMEM((2 * count, rows, head_dim), jnp.bfloat16),
            pltpu.VMEM((rows, 2 * count * head_dim), jnp.bfloat16),
        ],
        compiler_params=pltpu.CompilerParams(vmem_limit_bytes=40 * 2**20),
        name="output",
    )(table, *pieces, mine, other)


def one_head_per_device(*args):
    return attention_layer(*args)


def attention_layer(
    tokens, query_weight, key_weight, value_weight, output_weight, adapter_down, adapter_up
):
    tok_rows = tokens.shape[0]
    ctx_count = lax.axis_size("ctx")
    ctx_index = lax.axis_index("ctx")
    y_index = lax.axis_index("head")
    head_dim = D // HEADS
    slab_len = tok_rows * ctx_count
    plane = ctx_count // 4
    half = tok_rows // 2
    z_index, in_plane = ctx_index // plane, ctx_index % plane
    rank = adapter_down.shape[1]

    kept = lax.dynamic_slice_in_dim(tokens, y_index * half, half, 0)
    other = lax.dynamic_slice_in_dim(tokens, (1 - y_index) * half, half, 0)
    came = exchanged(other, "head", 1)
    shard = jnp.where(
        y_index == 0, jnp.concatenate([kept, came], 1), jnp.concatenate([came, kept], 1)
    )

    def spread(own):
        line = line_gather(own, plane)
        groups = []
        for piece in line:
            across = exchanged(piece, "ctx", 2)
            beside = exchanged(piece, "ctx", 1)
            groups.append([piece, beside, across, exchanged(across, "ctx", 1)])
        return groups

    slots = spread(shard)

    def swap(weight):
        return lax.all_to_all(weight, "ctx", split_axis=1, concat_axis=0, tiled=True)

    mine = [swap(weight) for weight in (query_weight, key_weight, value_weight)]
    others = [exchanged(weight, "head", 1) for weight in mine]

    down = jnp.pad(adapter_down.reshape(3 * rank, D).T, ((0, 0), (0, head_dim - 3 * rank)))
    up_mine = lax.dynamic_slice_in_dim(adapter_up, ctx_index * head_dim, head_dim, 2)
    up_pair = jnp.concatenate([up_mine, exchanged(up_mine, "head", 1)], 2)
    up = jnp.zeros((head_dim, 6 * head_dim), jnp.bfloat16)
    for which in range(3):
        up = lax.dynamic_update_slice(up, up_pair[which], (which * rank, which * 2 * head_dim))

    variant = jnp.array([0, 1, 2, 3], dtype=jnp.int32)
    local = jnp.arange(half, dtype=jnp.int32)
    inverse_freq = 10000.0 ** (-(jnp.arange(head_dim // 2, dtype=jnp.float32) * 2.0) / head_dim)
    places = [z * plane + (in_plane ^ variant) for z in line_sources(z_index)]
    parts, plan = [], []
    for first, last, split in GROUPS:
        rows_from = jnp.concatenate(places[first:last])[:, None] * tok_rows
        positions = (rows_from + y_index * half + local[None, :]).reshape(-1)
        angles = positions.astype(jnp.float32)[:, None] * inverse_freq[None, :]
        cosine, sine = jnp.cos(angles), jnp.sin(angles)
        cosine = jnp.concatenate([cosine, cosine], 1)
        sine = jnp.concatenate([-sine, sine], 1)
        pieces = [piece for slot in slots[first:last] for piece in slot]
        ready, cosine, sine, full_up = lax.optimization_barrier((down, cosine, sine, up))
        low = lower(pieces, ready)
        for kinds in split:
            weights = [mine[kind] for kind in kinds] + [others[kind] for kind in kinds]
            depth = 512 if len(kinds) == 2 else 1024
            own_part, peer_part = project(
                pieces, weights, kinds, low, full_up, cosine, sine, head_dim, depth
            )
            parts += [own_part, exchanged(peer_part, "head", 1)]
            plan.append((first, kinds))

    sources = jnp.concatenate(places)
    shift = jnp.where(y_index * ctx_count + ctx_index >= HEADS // 2, slab_len // 2, 0)
    sides = jnp.stack([y_index, 1 - y_index]).astype(jnp.int32)
    table = (sources[:, None] * 2 + sides[None, :]).reshape(-1)
    table = (table - shift // half) % (slab_len // half)
    table = jnp.concatenate([table, shift[None]]).astype(jnp.int32)
    result = flash(table, parts, plan, slab_len, head_dim, half)
    blocks = result.reshape(ctx_count, tok_rows, head_dim)
    mixed = lax.all_to_all(blocks, "ctx", split_axis=0, concat_axis=0, tiled=True)
    mixed_other = exchanged(mixed, "head", 1)

    pieces = [piece for group in spread(output_weight) for piece in group]
    heads_first = y_index * ctx_count
    out_table = jnp.concatenate([sources, heads_first[None]]).astype(jnp.int32)
    return output_project(out_table, pieces, mixed, mixed_other)


GROUPS = ((0, 3, ((0, 1), (2,))), (3, 4, ((0, 1, 2),)))


def one_head_fits(mesh):
    ctx_count, head_count = mesh.shape["ctx"], mesh.shape["head"]
    return ctx_count == GROUP_DEV and ctx_count // 4 == 4 and HEADS == ctx_count * head_count and head_count == 2


def solution(mesh):
    fits = one_head_fits(mesh)
    body = one_head_per_device if fits else per_device
    in_specs = (
        P("ctx", "head"),
        P("ctx", "head"),
        P("ctx", "head"),
        P("ctx", "head"),
        P("ctx", "head"),
        P(),
        P(None, None, "head"),
    )
    out_specs = P("ctx", "head")
    return jax.shard_map(
        body, mesh=mesh, in_specs=in_specs, out_specs=out_specs, check_vma=False
    )
```
